32 devices in a mesh: cx: 4 (over z), cy: 2 (over y), tp: 4 (over x, core).
Axes of the slice: x: 2, y: 2, z: 4, core: 2. Of those that a mesh axis runs over, the one named last changes fastest.
Arguments:
- neighbor_ids: int32 [16, 8, 128], P(('cx', 'cy'), 'tp'), may hold values from 0 to 1023
- decoder: bfloat16 [16, 64, 896], P(('cx', 'cy')), may hold values from -6 to 6
- table: bfloat16 [1024, 896], P(('cx', 'cy')), may hold values from -6 to 6
- attn_in: bfloat16 [6, 896, 896], P(None, ('cx', 'cy'), 'tp'), may hold values from -0.1875 to 0.1875
- attn_out: bfloat16 [2, 896, 896], P(None, 'tp', ('cx', 'cy')), may hold values from -0.1875 to 0.1875
- gains: float32 [3, 896], replicated, may hold values from 0.25 to 1.75
- w_up: bfloat16 [896, 3584], P(('cx', 'cy'), 'tp'), may hold values from -0.1875 to 0.1875
- w_down: bfloat16 [3584, 896], P('tp', ('cx', 'cy')), may hold values from -0.09375 to 0.09375
Outputs:
- encoded: bfloat16 [16, 8, 128, 896], P(('cx', 'cy'), 'tp')
The draws below stay inside these ranges and needn't reach their ends.
All inputs are finite; a program needn't handle non-finite values.
Results may differ from the reference program's by a relative error of at most 0.013.
Values may be sent and summed in bfloat16 or wider, within the bound.
A program may use at most 128 MiB of HBM per device.

```python
import math
import jax
import jax.numpy as jnp
import numpy as np
from jax import lax

D = 896
HD = 64
FF = 3584
VOCAB = 1024
L = 128
M = 64
SPANS = 16
NBR = 8


def set_ends(array, rng, low, largest):
    place = [jax.random.randint(jax.random.fold_in(rng, axis), (), 0, length) for axis, length in enumerate(array.shape)]
    main_axis = array.shape.index(max(array.shape))
    next_to = place[:main_axis] + [(place[main_axis] + 1) % array.shape[main_axis]] + place[main_axis + 1:]
    return array.at[tuple(place)].set(low).at[tuple(next_to)].set(largest)


def levels(rng, extent, split, least, high):
    loudness, own = 1.0, jax.random.fold_in(rng, 6)
    for axis_at, blocks in split:
        heights = jnp.exp(jax.random.uniform(jax.random.fold_in(own, axis_at), (blocks,), jnp.float32, least / len(split), high / len(split)))
        loudness = loudness * jnp.repeat(heights, extent[axis_at] // blocks).reshape([-1 if axis == axis_at else 1 for axis in range(len(extent))])
    return loudness


def rank_bounds(amount, lean):
    loads = [(1 << 20) // math.isqrt(standing ** lean) + 1 for standing in range(1, amount + 1)]
    deviation = 1 + sum(loads) // (1 << 30)
    return np.cumsum(np.array([max(1, weight // deviation) for weight in loads]))


def ranked(stream_key, shape, amount, slope):
    grid = rank_bounds(amount, slope)
    lot = jax.random.randint(jax.random.fold_in(stream_key, 1), shape, 0, int(grid[amount - 1]))
    grade = jnp.searchsorted(jnp.asarray(grid, jnp.int32), lot, side="right")
    return jax.random.permutation(jax.random.fold_in(stream_key, 2), amount)[grade].astype(jnp.int32)


def bell_draw(stream_key, shape, scale, limit, cuts=(), held_as=jnp.bfloat16):
    array = jax.random.normal(stream_key, shape, jnp.float32) * scale
    if len(cuts) > 0:
        array = levels(stream_key, shape, cuts, -0.22, 0.18) * array
    return jnp.clip(array, min=-limit, max=limit).astype(held_as)


def setup_inputs(seed: int = 0) -> dict:
    seeds = jax.random.split(jax.random.key(seed), 9)
    neighbor_ids = set_ends(ranked(seeds[0], (SPANS, NBR, L), VOCAB, 2), jax.random.fold_in(seeds[0], 3), 0, VOCAB - 1).astype(jnp.int32)
    decoder = bell_draw(seeds[1], (SPANS, M, D), 1.0, 6.0, ((0, 8),))
    table = bell_draw(seeds[2], (VOCAB, D), 1.0, 6.0, ((0, 8),))
    attn_in = bell_draw(seeds[3], (6, D, D), D ** -0.5, 0.1875, ((1, 8), (2, 4)))
    attn_out = bell_draw(seeds[4], (2, D, D), D ** -0.5, 0.1875, ((1, 4), (2, 8)))
    gains = jnp.clip(1.0 + 0.15 * jax.random.normal(seeds[5], (3, D), jnp.float32), 0.25, 1.75)
    w_up = bell_draw(seeds[6], (D, FF), D ** -0.5, 0.1875, ((0, 8), (1, 4)))
    w_down = bell_draw(seeds[7], (FF, D), FF ** -0.5, 0.09375, ((0, 4), (1, 8)))
    return {"neighbor_ids": neighbor_ids, "decoder": decoder, "table": table, "attn_in": attn_in, "attn_out": attn_out, "gains": gains, "w_up": w_up, "w_down": w_down}


def layer_norm(values, gain):
    middle = lax.optimization_barrier(jnp.mean(values, axis=-1, keepdims=True))
    centred = values - middle
    spread = lax.optimization_barrier(jnp.mean(centred * centred, axis=-1, keepdims=True))
    return (centred * lax.rsqrt(spread + 1e-05) * gain).astype(jnp.bfloat16)

def project(hidden, matrix):
    return jnp.dot(hidden, matrix, preferred_element_type=jnp.float32).astype(jnp.bfloat16)

def attend(query, key_rows, value_rows):
    batch, q_len, width = query.shape
    k_len = key_rows.shape[1]
    heads = width // HD
    q_heads = query.reshape(batch, q_len, heads, HD).astype(jnp.float32)
    k_heads = key_rows.reshape(batch, k_len, heads, HD).astype(jnp.float32)
    v_heads = value_rows.reshape(batch, k_len, heads, HD).astype(jnp.float32)
    scores = jnp.einsum('bqhd,bkhd->bhqk', q_heads, k_heads) * HD ** (-0.5)
    probs = jax.nn.softmax(scores, axis=-1).astype(jnp.bfloat16).astype(jnp.float32)
    mixed = jnp.einsum('bhqk,bkhd->bqhd', probs, v_heads)
    return mixed.reshape(batch, q_len, width).astype(jnp.bfloat16)

def reference(neighbor_ids, decoder, table, attn_in, attn_out, gains, w_up, w_down):

    def one_span(item):
        ids, dec = item
        x_zero = table[ids.reshape(-1)].astype(jnp.float32)
        h_one = layer_norm(x_zero, gains[0])
        query = project(h_one, attn_in[0]).reshape(NBR, L, D)
        keys = project(h_one, attn_in[1]).reshape(NBR, L, D)
        values = project(h_one, attn_in[2]).reshape(NBR, L, D)
        self_out = attend(query, keys, values).reshape(NBR * L, D)
        x_one = x_zero + jnp.dot(self_out, attn_out[0], preferred_element_type=jnp.float32)
        h_two = layer_norm(x_one, gains[1])
        cross_q = project(h_two, attn_in[3]).reshape(1, NBR * L, D)
        cross_k = project(dec, attn_in[4]).reshape(1, M, D)
        cross_v = project(dec, attn_in[5]).reshape(1, M, D)
        cross = attend(cross_q, cross_k, cross_v).reshape(NBR * L, D)
        x_two = x_one + jnp.dot(cross, attn_out[1], preferred_element_type=jnp.float32)
        h_three = layer_norm(x_two, gains[2])
        upward = jnp.dot(h_three, w_up, preferred_element_type=jnp.float32)
        act = jax.nn.gelu(upward, approximate=True).astype(jnp.bfloat16)
        mixed = jnp.dot(act, w_down, preferred_element_type=jnp.float32)
        return (x_two + mixed).astype(jnp.bfloat16).reshape(NBR, L, D)
    return lax.map(one_span, (neighbor_ids, decoder))
```

```python
import jax
import jax.numpy as jnp
from jax import lax
from jax.sharding import PartitionSpec as P

HD = 64


def layer_norm(values, gain):
    middle = jnp.mean(values, axis=-1, keepdims=True)
    centred = values - middle
    spread = jnp.mean(centred * centred, axis=-1, keepdims=True)
    return (centred * lax.rsqrt(spread + 1e-05) * gain).astype(jnp.bfloat16)


def project(hidden, matrix):
    return jnp.dot(hidden, matrix, preferred_element_type=jnp.float32).astype(jnp.bfloat16)


def attend(query, key_rows, value_rows):
    batch, q_len, width = query.shape
    k_len = key_rows.shape[1]
    heads = width // HD
    q_heads = query.reshape(batch, q_len, heads, HD)
    k_heads = key_rows.reshape(batch, k_len, heads, HD)
    v_heads = value_rows.reshape(batch, k_len, heads, HD)
    scores = jnp.einsum(
        "bqhd,bkhd->bhqk", q_heads, k_heads, preferred_element_type=jnp.float32
    ) * HD ** (-0.5)
    probs = jax.nn.softmax(scores, axis=-1).astype(jnp.bfloat16)
    mixed = jnp.einsum("bhqk,bkhd->bqhd", probs, v_heads, preferred_element_type=jnp.float32)
    return mixed.reshape(batch, q_len, width).astype(jnp.bfloat16)


def body(neighbor_ids, decoder, table, attn_in, attn_out, gains, w_up, w_down):
    rows, cols = attn_in.shape[1:]
    packed = jnp.concatenate([attn_in, attn_out.transpose(0, 2, 1)], axis=0)
    packed = packed.transpose(1, 0, 2).reshape(rows, -1)
    full_table, every_w, up_w, down_w = (
        lax.all_gather(table, ("cx", "cy"), axis=0, tiled=True),
        lax.all_gather(packed, ("cx", "cy", "tp"), axis=0, tiled=True),
        lax.all_gather(w_up, ("cx", "cy"), axis=0, tiled=True),
        lax.all_gather(w_down, ("cx", "cy"), axis=1, tiled=True),
    )
    spans, nbrs, length = neighbor_ids.shape
    width = full_table.shape[1]
    dec_len = decoder.shape[1]
    total = spans * nbrs * length
    dec_rows = decoder.reshape(spans * dec_len, width)
    x_zero = jnp.take(full_table, neighbor_ids.reshape(-1), axis=0).astype(jnp.float32)
    h_one = layer_norm(x_zero, gains[0])
    shards = lax.axis_size("tp")
    whole = every_w.reshape(-1, shards, rows, attn_in.shape[0] + attn_out.shape[0], cols)
    whole = whole.transpose(3, 0, 2, 1, 4).reshape(-1, width, width)
    in_full, out_full = whole[: attn_in.shape[0]], whole[attn_in.shape[0] :]
    query = project(h_one, in_full[0]).reshape(spans * nbrs, length, width)
    keys = project(h_one, in_full[1]).reshape(spans * nbrs, length, width)
    values = project(h_one, in_full[2]).reshape(spans * nbrs, length, width)
    self_out = attend(query, keys, values).reshape(total, width)
    x_one = x_zero + jnp.dot(self_out, out_full[0].T, preferred_element_type=jnp.float32)
    h_two = layer_norm(x_one, gains[1])
    cross_q = project(h_two, in_full[3]).reshape(spans, nbrs * length, width)
    cross_k = project(dec_rows, in_full[4]).reshape(spans, dec_len, width)
    cross_v = project(dec_rows, in_full[5]).reshape(spans, dec_len, width)
    cross = attend(cross_q, cross_k, cross_v).reshape(total, width)
    x_two = x_one + jnp.dot(cross, out_full[1].T, preferred_element_type=jnp.float32)
    h_three = layer_norm(x_two, gains[2])
    every = lax.all_gather(h_three, "tp", axis=0, tiled=True)
    upward = jnp.dot(every, up_w, preferred_element_type=jnp.float32)
    act = jax.nn.gelu(upward, approximate=True).astype(jnp.bfloat16)
    mixed = lax.psum_scatter(
        jnp.dot(act, down_w, preferred_element_type=jnp.float32).astype(jnp.bfloat16),
        "tp",
        scatter_dimension=0,
        tiled=True,
    ).astype(jnp.float32)
    return (x_two + mixed).astype(jnp.bfloat16).reshape(spans, nbrs, length, width)


def solution(mesh):
    in_specs = (
        P(("cx", "cy"), "tp", None),
        P(("cx", "cy"), None, None),
        P(("cx", "cy"), None),
        P(None, ("cx", "cy"), "tp"),
        P(None, "tp", ("cx", "cy")),
        P(),
        P(("cx", "cy"), "tp"),
        P("tp", ("cx", "cy")),
    )
    out_specs = P(("cx", "cy"), "tp", None, None)
    return jax.shard_map(body, mesh=mesh, in_specs=in_specs, out_specs=out_specs, check_vma=False)
```
